32 devices in a mesh: data: 1 (over z), hid: 4 (over y), vocab: 8 (over x, core).
Axes of the slice: x: 4, y: 4, z: 1, core: 2. Of those that a mesh axis runs over, the one named last changes fastest.
The devices are a block of a 4x4x8 slice.
Arguments:
- h_states: bfloat16 [1024, 6144], P('data', 'hid')
- w_head: bfloat16 [6144, 32768], P('hid', 'vocab')
- inv_temp: float32 [1024], P('data')
- tgt_ids: int32 [1024], P('data')
Outputs:
- output 1: float32 [1024, 32768], P('data', ('vocab', 'hid'))
- output 2: float32 [1024], P('data')
All inputs are finite; a program needn't handle non-finite values.
Results may differ from the reference program's by a relative error of at most 0.001.
Values are sent between devices in bfloat16 or wider.
A program may use at most 768 MiB of HBM per device.

```python
import jax
import jax.numpy as jnp
from jax import lax
import math

B = 1024
D = 6144
V = 32768


def setup_inputs(seed: int = 0, part: int = 0) -> dict:
    part_keys = jax.random.split(jax.random.fold_in(jax.random.key(seed), part), 5)
    shared_keys = jax.random.split(jax.random.key(seed + 1), 2)
    common_dir = jax.random.normal(shared_keys[0], (D,), jnp.float32)
    col_level = 140.0 - 2.5 * jnp.arange(V, dtype=jnp.float32) / V
    row_keys = jax.random.split(shared_keys[1], D // 128)
    dir_blocks = common_dir.reshape(D // 128, 128)

    def weight_block(block_args):
        blk_key, dir_part = block_args
        noise_blk = jax.random.normal(blk_key, (128, V), jnp.float32)
        w_part = noise_blk * (0.6 / math.sqrt(D)) + dir_part[:, None] * (col_level[None, :] / D)
        return w_part.astype(jnp.bfloat16)

    w_head = lax.map(weight_block, (row_keys, dir_blocks)).reshape(D, V)
    row_noise = jax.random.normal(part_keys[0], (B, D), jnp.float32)
    row_shift = jax.random.uniform(part_keys[1], (B,), jnp.float32, 1.0, 2.0)
    h_states = (row_noise + row_shift[:, None] * common_dir[None, :]).astype(jnp.bfloat16)
    inv_temp = jax.random.uniform(part_keys[2], (B,), jnp.float32, 0.7, 1.3)
    first_pick = jax.random.randint(part_keys[3], (B,), 0, V)
    second_pick = jax.random.randint(part_keys[4], (B,), 0, V)
    tgt_ids = jnp.maximum(first_pick, second_pick).at[0].set(0).at[1].set(V - 1)
    return {"h_states": h_states, "w_head": w_head, "inv_temp": inv_temp, "tgt_ids": tgt_ids}


def reference(h_states, w_head, inv_temp, tgt_ids):
    logits = jnp.dot(h_states, w_head, preferred_element_type=jnp.float32) * inv_temp[:, None]
    row_max = jnp.max(logits, axis=1, keepdims=True)
    exp_vals = jnp.exp(logits - row_max)
    row_sum = jnp.sum(exp_vals, axis=1, keepdims=True)
    prob_rows = exp_vals / row_sum
    cdf_table = jnp.cumsum(prob_rows, axis=1)
    cdf_at_tgt = jnp.take_along_axis(cdf_table, tgt_ids[:, None], axis=1)[:, 0]
    return (cdf_table, cdf_at_tgt)
```

```python
import functools

import jax
import jax.numpy as jnp
from jax import lax
from jax.experimental import pallas as pl
from jax.experimental.pallas import tpu as pltpu
from jax.sharding import PartitionSpec as P

MESH = pl.DeviceIdType.MESH
R = 128
LANES = 128
TRI = 256


def head_kernel(nh, nv, h_hbm, w_hbm, temp_ref, tgt_ref,
                c_hbm, scale_ref, off_ref, ctgt_ref,
                h_own, h_nb, w_sum, w_own, w_leaf, w_dir, s_send, s_recv, z_buf,
                stat_y, stat_x,
                ld_sem, hy_ss, hy_rs, hx_ss, hx_rs, leaf_ss, leaf_rs, dir_ss, dir_rs,
                sum_ss, sum_rs, sty_ss, sty_rs, stx_ss, stx_rs, out_sem):
    rows, depth = h_hbm.shape
    cb = w_hbm.shape[1] // nh
    hc = cb // 2
    nr = rows // R
    piece = rows // nv
    half = piece // 2

    me = lax.axis_index("hid")
    vi = lax.axis_index("vocab")
    up = lax.rem(me + 1, nh)
    dn = lax.rem(me + nh - 1, nh)
    far = lax.rem(me + 2, nh)
    nxt = lax.rem(vi + 2, nv)
    prv = lax.rem(vi + nv - 2, nv)
    opp = lax.rem(vi + 4, nv)
    mate = vi + 1 - 2 * lax.rem(vi, 2)

    def tok(d, part):
        return pl.ds(pl.multiple_of(d * cb + part * hc, LANES), hc)

    def rws(start, n):
        return pl.ds(pl.multiple_of(start, n), n)

    def rdma(src, dst, ss, rs, dev):
        return pltpu.make_async_remote_copy(
            src_ref=src, dst_ref=dst, send_sem=ss, recv_sem=rs,
            device_id=dev, device_id_type=MESH)

    loads = [
        pltpu.make_async_copy(h_hbm, h_own, ld_sem.at[0]),
        pltpu.make_async_copy(w_hbm.at[:, tok(dn, 0)], w_sum.at[0], ld_sem.at[1]),
        pltpu.make_async_copy(w_hbm.at[:, tok(up, 1)], w_sum.at[1], ld_sem.at[2]),
        pltpu.make_async_copy(
            w_hbm.at[:, pl.ds(pl.multiple_of(me * cb, LANES), cb)], w_own, ld_sem.at[3]),
    ]
    for c in loads:
        c.start()

    barrier = pltpu.get_barrier_semaphore()
    for j in range(1, nh):
        pl.semaphore_signal(barrier, inc=1, device_id={"hid": lax.rem(me + j, nh)},
                            device_id_type=MESH)
    for j in range(1, nv):
        pl.semaphore_signal(barrier, inc=1, device_id={"vocab": lax.rem(vi + j, nv)},
                            device_id_type=MESH)
    pl.semaphore_wait(barrier, nh - 1 + nv - 1)

    to_dn, to_up = {"hid": dn}, {"hid": up}
    mine = rws(vi * piece, piece)
    hy = [rdma(h_hbm.at[mine], h_nb.at[0, mine], hy_ss.at[0], hy_rs.at[0], to_dn),
          rdma(h_hbm.at[mine], h_nb.at[1, mine], hy_ss.at[1], hy_rs.at[1], to_up)]
    leaf = [rdma(w_hbm.at[:, tok(far, 0)], w_leaf.at[0], leaf_ss.at[0], leaf_rs.at[0], to_dn),
            rdma(w_hbm.at[:, tok(far, 1)], w_leaf.at[1], leaf_ss.at[1], leaf_rs.at[1], to_up)]
    direct = [rdma(w_hbm.at[:, tok(up, 0)], w_dir.at[0], dir_ss.at[0], dir_rs.at[0], to_up),
              rdma(w_hbm.at[:, tok(dn, 1)], w_dir.at[1], dir_ss.at[1], dir_rs.at[1], to_dn)]
    for c in hy + leaf:
        c.start()

    to_nxt, to_prv, to_mate = {"vocab": nxt}, {"vocab": prv}, {"vocab": mate}

    def hx(a, k, at, dev):
        return rdma(h_nb.at[a, at], h_nb.at[a, at], hx_ss.at[a, k], hx_rs.at[a, k], dev)

    from_prv = rws(prv * piece, piece)
    from_nxt = rws(nxt * piece, piece)
    opp_all = rws(opp * piece, piece)
    started = []

    def go(c):
        c.start()
        started.append(c)

    for a in range(2):
        hy[a].wait_recv()
        go(hx(a, 0, mine, to_nxt))
        go(hx(a, 1, mine, to_prv))
        go(hx(a, 4, mine, to_mate))
    for c in direct:
        c.start()

    for c in loads:
        c.wait()

    def own(i, _):
        at = rws(i * R, R)
        x = h_own[at]
        for p in range(2):
            s_send[p, at] = jnp.dot(x, w_sum[p], preferred_element_type=jnp.float32)
        for p in range(2):
            z_buf[at, p * hc:(p + 1) * hc] = jnp.dot(
                x, w_own[:, p * hc:(p + 1) * hc], preferred_element_type=jnp.float32)
        return 0

    lax.fori_loop(0, nr, own, 0)

    for a in range(2):
        hx(a, 0, from_prv, to_nxt).wait_recv()
        lo = rws(prv * piece, half)
        go(hx(a, 2, lo, to_nxt))
        go(hx(a, 5, from_prv, to_mate))
        hx(a, 1, from_nxt, to_prv).wait_recv()
        hi = rws(nxt * piece + half, half)
        go(hx(a, 3, hi, to_prv))
        go(hx(a, 6, from_nxt, to_mate))
    for a in range(2):
        hx(a, 2, rws(opp * piece, half), to_nxt).wait_recv()
        hx(a, 3, rws(opp * piece + half, half), to_prv).wait_recv()
        go(hx(a, 7, opp_all, to_mate))
    for a in range(2):
        for k in range(4, 8):
            hx(a, k, mine, to_mate).wait_recv()

    for c in leaf:
        c.wait_recv()

    def sum_copy(p, i):
        at = rws(i * R, R)
        return rdma(s_send.at[p, at], s_recv.at[p, at], sum_ss.at[p, i], sum_rs.at[p, i],
                    to_dn if p == 0 else to_up)

    def add_leaf(i, _):
        at = rws(i * R, R)
        for p in range(2):
            s_send[p, at] = s_send[p, at] + jnp.dot(
                h_nb[p, at], w_leaf[p], preferred_element_type=jnp.float32)
        for p in range(2):
            sum_copy(p, i).start()
        return 0

    lax.fori_loop(0, nr, add_leaf, 0)

    for c in direct:
        c.wait_recv()

    tri = (lax.broadcasted_iota(jnp.int32, (TRI, TRI), 0)
           <= lax.broadcasted_iota(jnp.int32, (TRI, TRI), 1)).astype(jnp.bfloat16)
    col = lax.broadcasted_iota(jnp.int32, (R, TRI), 1).astype(jnp.float32)
    lane = lax.broadcasted_iota(jnp.int32, (R, LANES), 1)
    first_tok = ((vi * nh + me) * cb).astype(jnp.float32)

    def out_copy(i):
        at = rws(i * R, R)
        return pltpu.make_async_copy(z_buf.at[at], c_hbm.at[at], out_sem.at[i])

    def by_row(v):
        return jnp.broadcast_to(v, (LANES, R)).T

    def softmax(i, _):
        at = rws(i * R, R)
        for p in range(2):
            sl = slice(p * hc, (p + 1) * hc)
            z_buf[at, sl] = z_buf[at, sl] + jnp.dot(
                h_nb[1 - p, at], w_dir[p], preferred_element_type=jnp.float32)
        temp = jnp.concatenate([by_row(temp_ref[pl.ds(i, 1)])] * (TRI // LANES), axis=1)
        tgt = jnp.concatenate(
            [by_row(tgt_ref[pl.ds(i, 1)].astype(jnp.float32) - first_tok)] * (TRI // LANES), axis=1)
        for p in range(2):
            sum_copy(p, i).wait_recv()
        m = None
        zs = []
        for b in range(cb // TRI):
            p, o = divmod(b * TRI, hc)
            z = (z_buf[at, b * TRI:(b + 1) * TRI] + s_recv[p, at, o:o + TRI]) * temp
            zs.append(z)
            m = z if m is None else jnp.maximum(m, z)
        m = jnp.max(m, axis=1, keepdims=True)
        carry = jnp.zeros((R, 1), jnp.float32)
        picked = jnp.zeros((R, TRI), jnp.float32)
        for b in range(cb // TRI):
            e = jnp.exp(zs[b] - m)
            picked = picked + jnp.where(col + float(b * TRI) <= tgt, e, 0.0)
            e1 = e.astype(jnp.bfloat16)
            r1 = e - e1.astype(jnp.float32)
            e2 = r1.astype(jnp.bfloat16)
            e3 = (r1 - e2.astype(jnp.float32)).astype(jnp.bfloat16)
            c = (jnp.dot(e3, tri, preferred_element_type=jnp.float32)
                 + jnp.dot(e2, tri, preferred_element_type=jnp.float32)
                 + jnp.dot(e1, tri, preferred_element_type=jnp.float32)) + carry
            z_buf[at, b * TRI:(b + 1) * TRI] = c
            carry = c[:, TRI - 1:TRI]
        out_copy(i).start()
        t = jnp.sum(picked, axis=1, keepdims=True)
        st = jnp.where(lane == 0, m, jnp.where(lane == 1, carry, jnp.where(lane == 2, t, 0.0))).T
        for k in range(3):
            stat_y[me, k, pl.ds(i, 1)] = st[k:k + 1]
        return 0

    lax.fori_loop(0, nr, softmax, 0)

    def sty(j):
        return rdma(stat_y.at[me], stat_y.at[me], sty_ss.at[j - 1], sty_rs.at[me],
                    {"hid": lax.rem(me + j, nh)})

    def stx(j):
        return rdma(stat_x.at[vi], stat_x.at[vi], stx_ss.at[j - 1], stx_rs.at[vi],
                    {"vocab": lax.rem(vi + j, nv)})

    for j in range(1, nh):
        sty(j).start()
    for j in range(1, nh):
        s = lax.rem(me + j, nh)
        rdma(stat_y.at[s], stat_y.at[s], sty_ss.at[j - 1], sty_rs.at[s], to_up).wait_recv()
    m_me = stat_y[me, 0]
    m_g = stat_y[0, 0]
    for j in range(1, nh):
        m_g = jnp.maximum(m_g, stat_y[j, 0])
    zero = jnp.zeros_like(m_g)
    s_g, t_g, pre = zero, zero, zero
    for j in range(nh):
        f = jnp.exp(stat_y[j, 0] - m_g)
        s_j = stat_y[j, 1] * f
        pre = pre + jnp.where(j < me, s_j, 0.0)
        s_g = s_g + s_j
        t_g = t_g + stat_y[j, 2] * f
    stat_x[vi, 0] = m_g
    stat_x[vi, 1] = s_g
    stat_x[vi, 2] = t_g
    for j in range(1, nv):
        stx(j).start()
    for j in range(1, nv):
        s = lax.rem(vi + j, nv)
        rdma(stat_x.at[s], stat_x.at[s], stx_ss.at[j - 1], stx_rs.at[s], to_nxt).wait_recv()
    big = stat_x[0, 0]
    for j in range(1, nv):
        big = jnp.maximum(big, stat_x[j, 0])
    tot, low, hit = zero, zero, zero
    for j in range(nv):
        f = jnp.exp(stat_x[j, 0] - big)
        s_j = stat_x[j, 1] * f
        low = low + jnp.where(j < vi, s_j, 0.0)
        tot = tot + s_j
        hit = hit + stat_x[j, 2] * f
    scale_ref[...] = jnp.exp(m_me - big) / tot
    off_ref[...] = (low + pre * jnp.exp(m_g - big)) / tot
    ctgt_ref[...] = hit / tot

    for c in hy + leaf + direct + started:
        c.wait_send()

    def drain(i, _):
        for p in range(2):
            sum_copy(p, i).wait_send()
        out_copy(i).wait()
        return 0

    lax.fori_loop(0, nr, drain, 0)
    for j in range(1, nh):
        sty(j).wait_send()
    for j in range(1, nv):
        stx(j).wait_send()


def solution(mesh):
    nh = mesh.shape["hid"]
    nv = mesh.shape["vocab"]

    def local_step(h, w, temp, tgt):
        rows, depth = h.shape
        cols = w.shape[1]
        cb = cols // nh
        hc = cb // 2
        nr = rows // R
        f32, bf16 = jnp.float32, jnp.bfloat16
        dma = pltpu.SemaphoreType.DMA
        vm = pl.BlockSpec(memory_space=pltpu.VMEM)
        hbm = pl.BlockSpec(memory_space=pl.ANY)
        row_stat = jax.ShapeDtypeStruct((nr, R), f32)
        c, scale, off, ctgt = pl.pallas_call(
            functools.partial(head_kernel, nh, nv),
            name="head",
            out_shape=(jax.ShapeDtypeStruct((rows, cb), f32), row_stat, row_stat, row_stat),
            in_specs=[hbm, hbm, vm, vm],
            out_specs=(hbm, vm, vm, vm),
            scratch_shapes=[
                pltpu.VMEM((rows, depth), bf16),
                pltpu.VMEM((2, rows, depth), bf16),
                pltpu.VMEM((2, depth, hc), bf16),
                pltpu.VMEM((depth, cb), bf16),
                pltpu.VMEM((2, depth, hc), bf16),
                pltpu.VMEM((2, depth, hc), bf16),
                pltpu.VMEM((2, rows, hc), f32),
                pltpu.VMEM((2, rows, hc), f32),
                pltpu.VMEM((rows, cb), f32),
                pltpu.VMEM((nh, 3, nr, R), f32),
                pltpu.VMEM((nv, 3, nr, R), f32),
                dma((4,)), dma((2,)), dma((2,)), dma((2, 8)), dma((2, 8)),
                dma((2,)), dma((2,)), dma((2,)), dma((2,)),
                dma((2, nr)), dma((2, nr)),
                dma((nh - 1,)), dma((nh,)), dma((nv - 1,)), dma((nv,)),
                dma((nr,)),
            ],
            cost_estimate=pl.CostEstimate(
                flops=2 * rows * depth * cols, bytes_accessed=2 * depth * (rows + cols) + 4 * rows * cb,
                transcendentals=rows * cb),
            compiler_params=pltpu.CompilerParams(
                collective_id=0, has_side_effects=True, vmem_limit_bytes=60 * 1024 * 1024),
        )(h, w, temp.reshape(nr, R), tgt.reshape(nr, R))
        cdf = c * scale.reshape(rows)[:, None] + off.reshape(rows)[:, None]
        return cdf, ctgt.reshape(rows)

    return jax.shard_map(
        local_step, mesh=mesh,
        in_specs=(P("data", "hid"), P("hid", "vocab"), P("data"), P("data")),
        out_specs=(P("data", ("vocab", "hid")), P("data")), check_vma=False)
```

```python
import functools

import jax
import jax.numpy as jnp
from jax import lax
from jax.experimental import pallas as pl
from jax.experimental.pallas import tpu as pltpu
from jax.sharding import PartitionSpec as P

MESH = pl.DeviceIdType.MESH
R = 128
LANES = 128
TRI = 256


def head_kernel(nh, nv, h_hbm, w_hbm, temp_hbm, tgt_hbm,
                z_buf, scale_ref, off_ref, hit_ref,
                h_own, h_nb, w_sum, w_own, w_leaf, w_dir, s_send, s_recv, temp_ref, tgt_ref,
                sy_a, sx_a, sy_b, sx_b,
                ld_sem, hy_ss, hy_rs, hx_ss, hx_rs, leaf_ss, leaf_rs, dir_ss, dir_rs,
                sum_ss, sum_rs, sty_ss, sty_rs, stx_ss, stx_rs):
    rows, depth = h_hbm.shape
    cb = w_hbm.shape[1] // nh
    hc = cb // 2
    nr = rows // R
    piece = rows // nv
    half = piece // 2

    me = lax.axis_index("hid")
    vi = lax.axis_index("vocab")
    up = lax.rem(me + 1, nh)
    dn = lax.rem(me + nh - 1, nh)
    far = lax.rem(me + 2, nh)
    nxt = lax.rem(vi + 2, nv)
    prv = lax.rem(vi + nv - 2, nv)
    opp = lax.rem(vi + 4, nv)
    mate = vi + 1 - 2 * lax.rem(vi, 2)

    def tok(d, part):
        return pl.ds(pl.multiple_of(d * cb + part * hc, LANES), hc)

    def rws(start, n):
        return pl.ds(pl.multiple_of(start, n), n)

    def rdma(src, dst, ss, rs, dev):
        return pltpu.make_async_remote_copy(
            src_ref=src, dst_ref=dst, send_sem=ss, recv_sem=rs,
            device_id=dev, device_id_type=MESH)

    loads = [
        pltpu.make_async_copy(h_hbm, h_own, ld_sem.at[0]),
        pltpu.make_async_copy(w_hbm.at[:, tok(dn, 0)], w_sum.at[0], ld_sem.at[1]),
        pltpu.make_async_copy(w_hbm.at[:, tok(up, 1)], w_sum.at[1], ld_sem.at[2]),
        pltpu.make_async_copy(
            w_hbm.at[:, pl.ds(pl.multiple_of(me * cb, LANES), cb)], w_own, ld_sem.at[3]),
        pltpu.make_async_copy(temp_hbm, temp_ref, ld_sem.at[4]),
        pltpu.make_async_copy(tgt_hbm, tgt_ref, ld_sem.at[5]),
    ]
    for c in loads:
        c.start()

    barrier = pltpu.get_barrier_semaphore()
    for j in range(1, nh):
        pl.semaphore_signal(barrier, inc=1, device_id={"hid": lax.rem(me + j, nh)},
                            device_id_type=MESH)
    for j in range(1, nv):
        pl.semaphore_signal(barrier, inc=1, device_id={"vocab": lax.rem(vi + j, nv)},
                            device_id_type=MESH)
    pl.semaphore_wait(barrier, nh - 1 + nv - 1)

    to_dn, to_up = {"hid": dn}, {"hid": up}
    mine = rws(vi * piece, piece)
    hy = [rdma(h_own.at[mine], h_nb.at[0, mine], hy_ss.at[0], hy_rs.at[0], to_dn),
          rdma(h_own.at[mine], h_nb.at[1, mine], hy_ss.at[1], hy_rs.at[1], to_up)]
    leaf = [rdma(w_hbm.at[:, tok(far, 0)], w_leaf.at[0], leaf_ss.at[0], leaf_rs.at[0], to_dn),
            rdma(w_hbm.at[:, tok(far, 1)], w_leaf.at[1], leaf_ss.at[1], leaf_rs.at[1], to_up)]
    direct = [rdma(w_hbm.at[:, tok(up, 0)], w_dir.at[0], dir_ss.at[0], dir_rs.at[0], to_up),
              rdma(w_hbm.at[:, tok(dn, 1)], w_dir.at[1], dir_ss.at[1], dir_rs.at[1], to_dn)]
    loads[0].wait()
    for c in hy + leaf:
        c.start()

    to_nxt, to_prv, to_mate = {"vocab": nxt}, {"vocab": prv}, {"vocab": mate}

    def hx(a, k, at, dev):
        return rdma(h_nb.at[a, at], h_nb.at[a, at], hx_ss.at[a, k], hx_rs.at[a, k], dev)

    from_prv = rws(prv * piece, piece)
    from_nxt = rws(nxt * piece, piece)
    opp_all = rws(opp * piece, piece)
    started = []

    def go(c):
        c.start()
        started.append(c)

    for a in range(2):
        hy[a].wait_recv()
        go(hx(a, 0, mine, to_nxt))
        go(hx(a, 1, mine, to_prv))
        go(hx(a, 4, mine, to_mate))
    for c in direct:
        c.start()

    for c in loads[1:]:
        c.wait()

    def own(i, _):
        at = rws(i * R, R)
        x = h_own[at]
        for p in range(2):
            s_send[p, at] = jnp.dot(x, w_sum[p], preferred_element_type=jnp.float32)
        for p in range(2):
            z_buf[at, p * hc:(p + 1) * hc] = jnp.dot(
                x, w_own[:, p * hc:(p + 1) * hc], preferred_element_type=jnp.float32)
        return 0

    lax.fori_loop(0, nr, own, 0)

    for a in range(2):
        hx(a, 0, from_prv, to_nxt).wait_recv()
        lo = rws(prv * piece, half)
        go(hx(a, 2, lo, to_nxt))
        go(hx(a, 5, from_prv, to_mate))
        hx(a, 1, from_nxt, to_prv).wait_recv()
        hi = rws(nxt * piece + half, half)
        go(hx(a, 3, hi, to_prv))
        go(hx(a, 6, from_nxt, to_mate))
    for a in range(2):
        hx(a, 2, rws(opp * piece, half), to_nxt).wait_recv()
        hx(a, 3, rws(opp * piece + half, half), to_prv).wait_recv()
        go(hx(a, 7, opp_all, to_mate))
    for a in range(2):
        for k in range(4, 8):
            hx(a, k, mine, to_mate).wait_recv()

    for c in leaf:
        c.wait_recv()

    def sum_copy(p, i):
        at = rws(i * R, R)
        return rdma(s_send.at[p, at], s_recv.at[p, at], sum_ss.at[p, i], sum_rs.at[p, i],
                    to_dn if p == 0 else to_up)

    def add_leaf(i, _):
        at = rws(i * R, R)
        for p in range(2):
            s_send[p, at] = s_send[p, at] + jnp.dot(
                h_nb[p, at], w_leaf[p], preferred_element_type=jnp.float32)
        for p in range(2):
            sum_copy(p, i).start()
        return 0

    lax.fori_loop(0, nr, add_leaf, 0)

    for c in direct:
        c.wait_recv()

    tri = (lax.broadcasted_iota(jnp.int32, (TRI, TRI), 0)
           <= lax.broadcasted_iota(jnp.int32, (TRI, TRI), 1)).astype(jnp.bfloat16)
    col = lax.broadcasted_iota(jnp.int32, (R, TRI), 1).astype(jnp.float32)
    lane = lax.broadcasted_iota(jnp.int32, (R, LANES), 1)
    first_tok = ((vi * nh + me) * cb).astype(jnp.float32)

    def by_row(v):
        return jnp.broadcast_to(v, (LANES, R)).T

    def softmax(i, sy, k):
        at = rws(i * R, R)
        for p in range(2):
            sl = slice(p * hc, (p + 1) * hc)
            z_buf[at, sl] = z_buf[at, sl] + jnp.dot(
                h_nb[1 - p, at], w_dir[p], preferred_element_type=jnp.float32)
        temp = jnp.concatenate([by_row(temp_ref[pl.ds(i, 1)])] * (TRI // LANES), axis=1)
        tgt = jnp.concatenate(
            [by_row(tgt_ref[pl.ds(i, 1)].astype(jnp.float32) - first_tok)] * (TRI // LANES), axis=1)
        for p in range(2):
            sum_copy(p, i).wait_recv()
        m = None
        zs = []
        for b in range(cb // TRI):
            p, o = divmod(b * TRI, hc)
            z = (z_buf[at, b * TRI:(b + 1) * TRI] + s_recv[p, at, o:o + TRI]) * temp
            zs.append(z)
            m = z if m is None else jnp.maximum(m, z)
        m = jnp.max(m, axis=1, keepdims=True)
        carry = jnp.zeros((R, 1), jnp.float32)
        picked = jnp.zeros((R, TRI), jnp.float32)
        for b in range(cb // TRI):
            e = jnp.exp(zs[b] - m)
            picked = picked + jnp.where(col + float(b * TRI) <= tgt, e, 0.0)
            e1 = e.astype(jnp.bfloat16)
            r1 = e - e1.astype(jnp.float32)
            e2 = r1.astype(jnp.bfloat16)
            e3 = (r1 - e2.astype(jnp.float32)).astype(jnp.bfloat16)
            c = (jnp.dot(e3, tri, preferred_element_type=jnp.float32)
                 + jnp.dot(e2, tri, preferred_element_type=jnp.float32)
                 + jnp.dot(e1, tri, preferred_element_type=jnp.float32)) + carry
            z_buf[at, b * TRI:(b + 1) * TRI] = c
            carry = c[:, TRI - 1:TRI]
        t = jnp.sum(picked, axis=1, keepdims=True)
        st = jnp.where(lane == 0, m, jnp.where(lane == 1, carry, jnp.where(lane == 2, t, 0.0))).T
        for q in range(3):
            sy[me, q, pl.ds(k, 1)] = st[q:q + 1]

    def sty(g, j):
        sy = (sy_a, sy_b)[g]
        return rdma(sy.at[me], sy.at[me], sty_ss.at[g, j - 1], sty_rs.at[g, me],
                    {"hid": lax.rem(me + j, nh)})

    def stx(g, j):
        sx = (sx_a, sx_b)[g]
        return rdma(sx.at[vi], sx.at[vi], stx_ss.at[g, j - 1], stx_rs.at[g, vi],
                    {"vocab": lax.rem(vi + j, nv)})

    def send_y(g):
        for j in range(1, nh):
            sty(g, j).start()

    def merge_y(g):
        sy, sx = (sy_a, sy_b)[g], (sx_a, sx_b)[g]
        for j in range(1, nh):
            s = lax.rem(me + j, nh)
            rdma(sy.at[s], sy.at[s], sty_ss.at[g, j - 1], sty_rs.at[g, s], to_up).wait_recv()
        m_g = sy[0, 0]
        for j in range(1, nh):
            m_g = jnp.maximum(m_g, sy[j, 0])
        zero = jnp.zeros_like(m_g)
        s_g, t_g, pre = zero, zero, zero
        for j in range(nh):
            f = jnp.exp(sy[j, 0] - m_g)
            s_j = sy[j, 1] * f
            pre = pre + jnp.where(j < me, s_j, 0.0)
            s_g = s_g + s_j
            t_g = t_g + sy[j, 2] * f
        sx[vi, 0] = m_g
        sx[vi, 1] = s_g
        sx[vi, 2] = t_g
        for j in range(1, nv):
            stx(g, j).start()
        return m_g, pre

    def merge_x(g, m_g, pre, out):
        sy, sx = (sy_a, sy_b)[g], (sx_a, sx_b)[g]
        for j in range(1, nv):
            s = lax.rem(vi + j, nv)
            rdma(sx.at[s], sx.at[s], stx_ss.at[g, j - 1], stx_rs.at[g, s], to_nxt).wait_recv()
        big = sx[0, 0]
        for j in range(1, nv):
            big = jnp.maximum(big, sx[j, 0])
        zero = jnp.zeros_like(big)
        tot, low, hit = zero, zero, zero
        for j in range(nv):
            f = jnp.exp(sx[j, 0] - big)
            s_j = sx[j, 1] * f
            low = low + jnp.where(j < vi, s_j, 0.0)
            tot = tot + s_j
            hit = hit + sx[j, 2] * f
        scale_ref[out] = jnp.exp(sy[me, 0] - big) / tot
        off_ref[out] = (low + pre * jnp.exp(m_g - big)) / tot
        hit_ref[out] = hit / tot

    last = nr - 1
    for q in range(3):
        sy_a[me, q, last:nr] = jnp.zeros((1, R), jnp.float32)

    def block(i, _):
        softmax(i, sy_a, i)
        return 0

    lax.fori_loop(0, last, block, 0)
    send_y(0)
    softmax(last, sy_b, 0)
    send_y(1)
    got_a = merge_y(0)

    for c in hy + leaf + direct + started:
        c.wait_send()

    def drain(i, _):
        for p in range(2):
            sum_copy(p, i).wait_send()
        return 0

    lax.fori_loop(0, nr, drain, 0)
    got_b = merge_y(1)
    merge_x(0, *got_a, slice(None))
    merge_x(1, *got_b, slice(last, nr))
    for g in range(2):
        for j in range(1, nh):
            sty(g, j).wait_send()
        for j in range(1, nv):
            stx(g, j).wait_send()


def final_kernel(c_ref, scale_ref, off_ref, hit_ref, out_hbm, hit_out, buf, sem):
    nr = scale_ref.shape[0]

    def by_row(v):
        return jnp.broadcast_to(v, (LANES, R)).T

    def out_copy(i):
        at = pl.ds(pl.multiple_of(i * R, R), R)
        return pltpu.make_async_copy(buf.at[at], out_hbm.at[at], sem.at[i])

    def block(i, _):
        a = by_row(scale_ref[pl.ds(i, 1)])
        b = by_row(off_ref[pl.ds(i, 1)])
        at = pl.ds(pl.multiple_of(i * R, R), R)
        for j in range(c_ref.shape[1] // LANES):
            sl = slice(j * LANES, (j + 1) * LANES)
            buf[at, sl] = c_ref[at, sl] * a + b
        out_copy(i).start()
        return 0

    lax.fori_loop(0, nr, block, 0)
    hit_out[...] = hit_ref[...]

    def drain(i, _):
        out_copy(i).wait()
        return 0

    lax.fori_loop(0, nr, drain, 0)


def solution(mesh):
    nh = mesh.shape["hid"]
    nv = mesh.shape["vocab"]

    def local_step(h, w, temp, tgt):
        rows, depth = h.shape
        cols = w.shape[1]
        cb = cols // nh
        hc = cb // 2
        nr = rows // R
        f32, bf16 = jnp.float32, jnp.bfloat16
        dma = pltpu.SemaphoreType.DMA
        vm = pl.BlockSpec(memory_space=pltpu.VMEM)
        hbm = pl.BlockSpec(memory_space=pltpu.HBM)
        row_stat = jax.ShapeDtypeStruct((nr, R), f32)
        table = jax.ShapeDtypeStruct((rows, cb), f32)
        c, scale, off, hit = pl.pallas_call(
            functools.partial(head_kernel, nh, nv),
            name="head",
            out_shape=(table, row_stat, row_stat, row_stat),
            in_specs=[hbm, hbm, hbm, hbm],
            out_specs=(vm, vm, vm, vm),
            scratch_shapes=[
                pltpu.VMEM((rows, depth), bf16),
                pltpu.VMEM((2, rows, depth), bf16),
                pltpu.VMEM((2, depth, hc), bf16),
                pltpu.VMEM((depth, cb), bf16),
                pltpu.VMEM((2, depth, hc), bf16),
                pltpu.VMEM((2, depth, hc), bf16),
                pltpu.VMEM((2, rows, hc), f32),
                pltpu.VMEM((2, rows, hc), f32),
                pltpu.VMEM((nr, R), f32),
                pltpu.VMEM((nr, R), jnp.int32),
                pltpu.VMEM((nh, 3, nr, R), f32),
                pltpu.VMEM((nv, 3, nr, R), f32),
                pltpu.VMEM((nh, 3, 1, R), f32),
                pltpu.VMEM((nv, 3, 1, R), f32),
                dma((6,)), dma((2,)), dma((2,)), dma((2, 8)), dma((2, 8)),
                dma((2,)), dma((2,)), dma((2,)), dma((2,)),
                dma((2, nr)), dma((2, nr)),
                dma((2, nh - 1)), dma((2, nh)), dma((2, nv - 1)), dma((2, nv)),
            ],
            cost_estimate=pl.CostEstimate(
                flops=2 * rows * depth * cols, bytes_accessed=2 * depth * (rows + cols) + 4 * rows * cb,
                transcendentals=rows * cb),
            compiler_params=pltpu.CompilerParams(
                collective_id=0, has_side_effects=True, vmem_limit_bytes=44 * 1024 * 1024),
        )(*[pltpu.with_memory_space_constraint(x, pltpu.HBM)
            for x in (h, w, temp.reshape(nr, R), tgt.reshape(nr, R))])
        cdf, ctgt = pl.pallas_call(
            final_kernel,
            name="final",
            out_shape=(table, row_stat),
            in_specs=[vm, vm, vm, vm],
            out_specs=(hbm, vm),
            scratch_shapes=[pltpu.VMEM((rows, cb), f32), dma((nr,))],
            compiler_params=pltpu.CompilerParams(vmem_limit_bytes=16 * 1024 * 1024),
        )(c, scale, off, hit)
        return cdf, ctgt.reshape(rows)

    return jax.shard_map(
        local_step, mesh=mesh,
        in_specs=(P("data", "hid"), P("hid", "vocab"), P("data"), P("data")),
        out_specs=(P("data", ("vocab", "hid")), P("data")), check_vma=False)
```

```python
import functools

import jax
import jax.numpy as jnp
from jax import lax
from jax.experimental import pallas as pl
from jax.experimental.pallas import tpu as pltpu
from jax.sharding import PartitionSpec as P

MESH = pl.DeviceIdType.MESH
R = 128
LANES = 128
NC = 1
TRI = 256


def head_kernel(nh, nv, h_hbm, w_hbm, temp_hbm, tgt_hbm,
                z_buf, hit_ref,
                h_own, h_nb, w_sum, w_own, w_leaf, w_dir, s_send, s_recv, temp_ref, tgt_ref,
                sy_a, sx_a, s_all,
                ld_sem, hy_ss, hy_rs, hx_ss, hx_rs, leaf_ss, leaf_rs, dir_ss, dir_rs,
                sum_ss, sum_rs, sty_ss, sty_rs, stx_ss, stx_rs, all_ss, all_rs):
    rows, depth = h_hbm.shape
    cb = w_hbm.shape[1] // nh
    hc = cb // 2
    nr = rows // R
    piece = rows // nv
    half = piece // 2

    me = lax.axis_index("hid")
    vi = lax.axis_index("vocab")
    up = lax.rem(me + 1, nh)
    dn = lax.rem(me + nh - 1, nh)
    far = lax.rem(me + 2, nh)
    nxt = lax.rem(vi + 2, nv)
    prv = lax.rem(vi + nv - 2, nv)
    opp = lax.rem(vi + 4, nv)
    mate = vi + 1 - 2 * lax.rem(vi, 2)

    def tok(d, part):
        return pl.ds(pl.multiple_of(d * cb + part * hc, LANES), hc)

    def rws(start, n):
        return pl.ds(pl.multiple_of(start, n), n)

    def rdma(src, dst, ss, rs, dev):
        return pltpu.make_async_remote_copy(
            src_ref=src, dst_ref=dst, send_sem=ss, recv_sem=rs,
            device_id=dev, device_id_type=MESH)

    loads = [
        pltpu.make_async_copy(h_hbm, h_own, ld_sem.at[0]),
        pltpu.make_async_copy(w_hbm.at[:, tok(dn, 0)], w_sum.at[0], ld_sem.at[1]),
        pltpu.make_async_copy(w_hbm.at[:, tok(up, 1)], w_sum.at[1], ld_sem.at[2]),
        pltpu.make_async_copy(
            w_hbm.at[:, pl.ds(pl.multiple_of(me * cb, LANES), cb)], w_own, ld_sem.at[3]),
        pltpu.make_async_copy(temp_hbm, temp_ref, ld_sem.at[4]),
        pltpu.make_async_copy(tgt_hbm, tgt_ref, ld_sem.at[5]),
    ]
    for c in loads:
        c.start()

    barrier = pltpu.get_barrier_semaphore()
    for j in range(1, nh):
        pl.semaphore_signal(barrier, inc=1, device_id={"hid": lax.rem(me + j, nh)},
                            device_id_type=MESH)
    for j in range(1, nv):
        pl.semaphore_signal(barrier, inc=1, device_id={"vocab": lax.rem(vi + j, nv)},
                            device_id_type=MESH)
    pl.semaphore_wait(barrier, nh - 1 + nv - 1)

    to_dn, to_up = {"hid": dn}, {"hid": up}
    mine = rws(vi * piece, piece)
    hy = [rdma(h_own.at[mine], h_nb.at[0, mine], hy_ss.at[0], hy_rs.at[0], to_dn),
          rdma(h_own.at[mine], h_nb.at[1, mine], hy_ss.at[1], hy_rs.at[1], to_up)]
    leaf = [rdma(w_hbm.at[:, tok(far, 0)], w_leaf.at[0], leaf_ss.at[0], leaf_rs.at[0], to_dn),
            rdma(w_hbm.at[:, tok(far, 1)], w_leaf.at[1], leaf_ss.at[1], leaf_rs.at[1], to_up)]
    direct = [rdma(w_hbm.at[:, tok(up, 0)], w_dir.at[0], dir_ss.at[0], dir_rs.at[0], to_up),
              rdma(w_hbm.at[:, tok(dn, 1)], w_dir.at[1], dir_ss.at[1], dir_rs.at[1], to_dn)]
    loads[0].wait()
    for c in hy + leaf:
        c.start()

    to_nxt, to_prv, to_mate = {"vocab": nxt}, {"vocab": prv}, {"vocab": mate}

    def hx(a, k, at, dev):
        return rdma(h_nb.at[a, at], h_nb.at[a, at], hx_ss.at[a, k], hx_rs.at[a, k], dev)

    from_prv = rws(prv * piece, piece)
    from_nxt = rws(nxt * piece, piece)
    opp_all = rws(opp * piece, piece)
    started = []

    def go(c):
        c.start()
        started.append(c)

    for a in range(2):
        hy[a].wait_recv()
        go(hx(a, 0, mine, to_nxt))
        go(hx(a, 1, mine, to_prv))
        go(hx(a, 4, mine, to_mate))
    for c in direct:
        c.start()

    for c in loads[1:]:
        c.wait()

    def own(i, _):
        at = rws(i * R, R)
        x = h_own[at]
        for p in range(2):
            s_send[p, at] = jnp.dot(x, w_sum[p], preferred_element_type=jnp.float32)
        for p in range(2):
            z_buf[at, p * hc:(p + 1) * hc] = jnp.dot(
                x, w_own[:, p * hc:(p + 1) * hc], preferred_element_type=jnp.float32)
        return 0

    lax.fori_loop(0, nr, own, 0)

    for a in range(2):
        hx(a, 0, from_prv, to_nxt).wait_recv()
        lo = rws(prv * piece, half)
        go(hx(a, 2, lo, to_nxt))
        go(hx(a, 5, from_prv, to_mate))
        hx(a, 1, from_nxt, to_prv).wait_recv()
        hi = rws(nxt * piece + half, half)
        go(hx(a, 3, hi, to_prv))
        go(hx(a, 6, from_nxt, to_mate))
    for a in range(2):
        hx(a, 2, rws(opp * piece, half), to_nxt).wait_recv()
        hx(a, 3, rws(opp * piece + half, half), to_prv).wait_recv()
        go(hx(a, 7, opp_all, to_mate))
    for a in range(2):
        for k in range(4, 8):
            hx(a, k, mine, to_mate).wait_recv()

    for c in leaf:
        c.wait_recv()

    def sum_copy(p, i):
        at = rws(i * R, R)
        return rdma(s_send.at[p, at], s_recv.at[p, at], sum_ss.at[p, i], sum_rs.at[p, i],
                    to_dn if p == 0 else to_up)

    def add_leaf(i, _):
        at = rws(i * R, R)
        for p in range(2):
            s_send[p, at] = s_send[p, at] + jnp.dot(
                h_nb[p, at], w_leaf[p], preferred_element_type=jnp.float32)
        for p in range(2):
            sum_copy(p, i).start()
        return 0

    lax.fori_loop(0, nr, add_leaf, 0)

    for c in direct:
        c.wait_recv()

    tri = (lax.broadcasted_iota(jnp.int32, (TRI, TRI), 0)
           <= lax.broadcasted_iota(jnp.int32, (TRI, TRI), 1)).astype(jnp.bfloat16)
    col = lax.broadcasted_iota(jnp.int32, (R, TRI), 1).astype(jnp.float32)
    lane = lax.broadcasted_iota(jnp.int32, (R, LANES), 1)
    first_tok = ((vi * nh + me) * cb).astype(jnp.float32)

    def by_row(v):
        return jnp.broadcast_to(v, (LANES, R)).T

    def finish(start, scale, off):
        a, b = by_row(scale), by_row(off)
        for j in range(cb // LANES):
            sl = slice(j * LANES, (j + 1) * LANES)
            z_buf[start:start + R, sl] = z_buf[start:start + R, sl] * a + b

    def softmax(i, sy, slot, k):
        at = rws(i * R, R)
        for p in range(2):
            sl = slice(p * hc, (p + 1) * hc)
            z_buf[at, sl] = z_buf[at, sl] + jnp.dot(
                h_nb[1 - p, at], w_dir[p], preferred_element_type=jnp.float32)
        temp = jnp.concatenate([by_row(temp_ref[pl.ds(i, 1)])] * (TRI // LANES), axis=1)
        tgt = jnp.concatenate(
            [by_row(tgt_ref[pl.ds(i, 1)].astype(jnp.float32) - first_tok)] * (TRI // LANES), axis=1)
        for p in range(2):
            sum_copy(p, i).wait_recv()
        m = None
        zs = []
        for b in range(cb // TRI):
            p, o = divmod(b * TRI, hc)
            z = (z_buf[at, b * TRI:(b + 1) * TRI] + s_recv[p, at, o:o + TRI]) * temp
            zs.append(z)
            m = z if m is None else jnp.maximum(m, z)
        m = jnp.max(m, axis=1, keepdims=True)
        carry = jnp.zeros((R, 1), jnp.float32)
        picked = jnp.zeros((R, TRI), jnp.float32)
        for b in range(cb // TRI):
            e = jnp.exp(zs[b] - m)
            picked = picked + jnp.where(col + float(b * TRI) <= tgt, e, 0.0)
            e1 = e.astype(jnp.bfloat16)
            r1 = e - e1.astype(jnp.float32)
            e2 = r1.astype(jnp.bfloat16)
            e3 = (r1 - e2.astype(jnp.float32)).astype(jnp.bfloat16)
            c = (jnp.dot(e3, tri, preferred_element_type=jnp.float32)
                 + jnp.dot(e2, tri, preferred_element_type=jnp.float32)
                 + jnp.dot(e1, tri, preferred_element_type=jnp.float32)) + carry
            z_buf[at, b * TRI:(b + 1) * TRI] = c
            carry = c[:, TRI - 1:TRI]
        t = jnp.sum(picked, axis=1, keepdims=True)
        st = jnp.where(lane == 0, m, jnp.where(lane == 1, carry, jnp.where(lane == 2, t, 0.0))).T
        for q in range(3):
            sy[slot, q, pl.ds(k, 1)] = st[q:q + 1]

    def sty(j):
        return rdma(sy_a.at[me], sy_a.at[me], sty_ss.at[j - 1], sty_rs.at[me],
                    {"hid": lax.rem(me + j, nh)})

    def stx(j):
        return rdma(sx_a.at[vi], sx_a.at[vi], stx_ss.at[j - 1], stx_rs.at[vi],
                    {"vocab": lax.rem(vi + j, nv)})

    def merge_y():
        for j in range(1, nh):
            s = lax.rem(me + j, nh)
            rdma(sy_a.at[s], sy_a.at[s], sty_ss.at[j - 1], sty_rs.at[s], to_up).wait_recv()
        m_g = sy_a[0, 0]
        for j in range(1, nh):
            m_g = jnp.maximum(m_g, sy_a[j, 0])
        zero = jnp.zeros_like(m_g)
        s_g, t_g, pre = zero, zero, zero
        for j in range(nh):
            f = jnp.exp(sy_a[j, 0] - m_g)
            s_j = sy_a[j, 1] * f
            pre = pre + jnp.where(j < me, s_j, 0.0)
            s_g = s_g + s_j
            t_g = t_g + sy_a[j, 2] * f
        sx_a[vi, 0] = m_g
        sx_a[vi, 1] = s_g
        sx_a[vi, 2] = t_g
        for j in range(1, nv):
            stx(j).start()
        return m_g, pre

    def merge_x(m_g, pre):
        for j in range(1, nv):
            s = lax.rem(vi + j, nv)
            rdma(sx_a.at[s], sx_a.at[s], stx_ss.at[j - 1], stx_rs.at[s], to_nxt).wait_recv()
        big = sx_a[0, 0]
        for j in range(1, nv):
            big = jnp.maximum(big, sx_a[j, 0])
        zero = jnp.zeros_like(big)
        tot, low, hit = zero, zero, zero
        for j in range(nv):
            f = jnp.exp(sx_a[j, 0] - big)
            s_j = sx_a[j, 1] * f
            low = low + jnp.where(j < vi, s_j, 0.0)
            tot = tot + s_j
            hit = hit + sx_a[j, 2] * f
        scale = jnp.exp(sy_a[me, 0] - big) / tot
        off = (low + pre * jnp.exp(m_g - big)) / tot
        hit_ref[...] = hit / tot
        for i in range(last):
            finish(i * R, scale[i:i + 1], off[i:i + 1])

    nd = nv * nh
    own_slot = vi * nh + me

    def peer(k):
        return lax.rem(vi + k // nh, nv), lax.rem(me + lax.rem(k, nh), nh)

    def sta(k):
        v, h = peer(k)
        return rdma(s_all.at[own_slot], s_all.at[own_slot], all_ss.at[k], all_rs.at[own_slot],
                    {"hid": h, "vocab": v})

    def send_all(k, _):
        sta(k).start()
        return 0

    def hear_all(k, _):
        v, h = peer(k)
        s = v * nh + h
        rdma(s_all.at[s], s_all.at[s], all_ss.at[k], all_rs.at[s], to_up).wait_recv()
        return 0

    def sent_all(k, _):
        sta(k).wait_send()
        return 0

    def merge_all():
        big = s_all[0, 0]
        for j in range(1, nd):
            big = jnp.maximum(big, s_all[j, 0])
        zero = jnp.zeros_like(big)
        tot, low, hit = zero, zero, zero
        for j in range(nd):
            f = jnp.exp(s_all[j, 0] - big)
            s_j = s_all[j, 1] * f
            low = low + jnp.where(j < own_slot, s_j, 0.0)
            tot = tot + s_j
            hit = hit + s_all[j, 2] * f
        hit_ref[last:nr] = hit / tot
        finish(last * R, jnp.exp(s_all[own_slot, 0] - big) / tot, low / tot)

    last = nr - 1
    for q in range(3):
        sy_a[me, q, last:nr] = jnp.zeros((1, R), jnp.float32)

    def block(i, _):
        softmax(i, sy_a, me, i)
        return 0

    lax.fori_loop(0, last, block, 0)
    for j in range(1, nh):
        sty(j).start()
    softmax(last, s_all, own_slot, 0)
    lax.fori_loop(1, nd, send_all, 0)
    got = merge_y()

    for c in hy + leaf + direct + started:
        c.wait_send()

    def drain(i, _):
        for p in range(2):
            sum_copy(p, i).wait_send()
        return 0

    lax.fori_loop(0, nr, drain, 0)
    merge_x(*got)
    lax.fori_loop(1, nd, hear_all, 0)
    merge_all()
    for j in range(1, nh):
        sty(j).wait_send()
    for j in range(1, nv):
        stx(j).wait_send()
    lax.fori_loop(1, nd, sent_all, 0)


def store_kernel(nc, c_ref, hit_ref, out_hbm, hit_hbm, sem):
    rows = c_ref.shape[0] // nc
    copies = [pltpu.make_async_copy(c_ref.at[i * rows:(i + 1) * rows],
                                    out_hbm.at[i * rows:(i + 1) * rows], sem.at[i])
              for i in range(nc)]
    copies.append(pltpu.make_async_copy(hit_ref, hit_hbm, sem.at[nc]))
    for c in copies:
        c.start()
    for c in copies:
        c.wait()


def solution(mesh):
    nh = mesh.shape["hid"]
    nv = mesh.shape["vocab"]

    def local_step(h, w, temp, tgt):
        rows, depth = h.shape
        cols = w.shape[1]
        cb = cols // nh
        hc = cb // 2
        nr = rows // R
        f32, bf16 = jnp.float32, jnp.bfloat16
        dma = pltpu.SemaphoreType.DMA
        vm = pl.BlockSpec(memory_space=pltpu.VMEM)
        hbm = pl.BlockSpec(memory_space=pltpu.HBM)
        row_stat = jax.ShapeDtypeStruct((nr, R), f32)
        cdf_out = jax.ShapeDtypeStruct((rows, cb), f32)
        table, hit = pl.pallas_call(
            functools.partial(head_kernel, nh, nv),
            name="head",
            out_shape=(cdf_out, row_stat),
            in_specs=[hbm, hbm, hbm, hbm],
            out_specs=(vm, vm),
            scratch_shapes=[
                pltpu.VMEM((rows, depth), bf16),
                pltpu.VMEM((2, rows, depth), bf16),
                pltpu.VMEM((2, depth, hc), bf16),
                pltpu.VMEM((depth, cb), bf16),
                pltpu.VMEM((2, depth, hc), bf16),
                pltpu.VMEM((2, depth, hc), bf16),
                pltpu.VMEM((2, rows, hc), f32),
                pltpu.VMEM((2, rows, hc), f32),
                pltpu.VMEM((nr, R), f32),
                pltpu.VMEM((nr, R), jnp.int32),
                pltpu.VMEM((nh, 3, nr, R), f32),
                pltpu.VMEM((nv, 3, nr, R), f32),
                pltpu.VMEM((nh * nv, 3, 1, R), f32),
                dma((6,)), dma((2,)), dma((2,)), dma((2, 8)), dma((2, 8)),
                dma((2,)), dma((2,)), dma((2,)), dma((2,)),
                dma((2, nr)), dma((2, nr)),
                dma((nh - 1,)), dma((nh,)), dma((nv - 1,)), dma((nv,)), dma((nh * nv,)), dma((nh * nv,)),
            ],
            cost_estimate=pl.CostEstimate(
                flops=2 * rows * depth * cols, bytes_accessed=2 * depth * (rows + cols) + 4 * rows * cb,
                transcendentals=rows * cb),
            compiler_params=pltpu.CompilerParams(
                collective_id=0, has_side_effects=True, vmem_limit_bytes=44 * 1024 * 1024),
        )(*[pltpu.with_memory_space_constraint(x, pltpu.HBM)
            for x in (h, w, temp.reshape(nr, R), tgt.reshape(nr, R))])
        cdf, ctgt = pl.pallas_call(
            functools.partial(store_kernel, NC),
            name="store",
            out_shape=(cdf_out, row_stat),
            in_specs=[vm, vm],
            out_specs=(hbm, hbm),
            scratch_shapes=[dma((NC + 1,))],
            compiler_params=pltpu.CompilerParams(vmem_limit_bytes=4 * 1024 * 1024),
        )(table, hit)
        return cdf, ctgt.reshape(rows)

    return jax.shard_map(
        local_step, mesh=mesh,
        in_specs=(P("data", "hid"), P("hid", "vocab"), P("data"), P("data")),
        out_specs=(P("data", ("vocab", "hid")), P("data")), check_vma=False)
```

```python
import functools

import jax
import jax.numpy as jnp
from jax import lax
from jax.experimental import pallas as pl
from jax.experimental.pallas import tpu as pltpu
from jax.sharding import PartitionSpec as P

MESH = pl.DeviceIdType.MESH
R = 128
LANES = 128
NC = 1
NB = 2
TRI = 256


def head_kernel(nh, nv, h_hbm, w_hbm, temp_hbm, tgt_hbm,
                z_buf, hit_ref,
                h_own, h_nb, w_sum, w_own, w_leaf, w_dir, s_send, s_recv, temp_ref, tgt_ref,
                sx_a, sy_out, sy_a, s_all,
                ld_sem, hy_ss, hy_rs, hx_ss, hx_rs, leaf_ss, leaf_rs, dir_ss, dir_rs,
                sum_ss, sum_rs, sty_ss, sty_rs, stx_ss, stx_rs, all_ss, all_rs):
    rows, depth = h_hbm.shape
    cb = w_hbm.shape[1] // nh
    hc = cb // 2
    nr = rows // R
    piece = rows // nv
    half = piece // 2

    me = lax.axis_index("hid")
    vi = lax.axis_index("vocab")
    up = lax.rem(me + 1, nh)
    dn = lax.rem(me + nh - 1, nh)
    far = lax.rem(me + 2, nh)
    nxt = lax.rem(vi + 2, nv)
    prv = lax.rem(vi + nv - 2, nv)
    opp = lax.rem(vi + 4, nv)
    mate = vi + 1 - 2 * lax.rem(vi, 2)

    def tok(d, part):
        return pl.ds(pl.multiple_of(d * cb + part * hc, LANES), hc)

    def rws(start, n):
        return pl.ds(pl.multiple_of(start, n), n)

    def rdma(src, dst, ss, rs, dev):
        return pltpu.make_async_remote_copy(
            src_ref=src, dst_ref=dst, send_sem=ss, recv_sem=rs,
            device_id=dev, device_id_type=MESH)

    loads = [
        pltpu.make_async_copy(h_hbm, h_own, ld_sem.at[0]),
        pltpu.make_async_copy(w_hbm.at[:, tok(dn, 0)], w_sum.at[0], ld_sem.at[1]),
        pltpu.make_async_copy(w_hbm.at[:, tok(up, 1)], w_sum.at[1], ld_sem.at[2]),
        pltpu.make_async_copy(
            w_hbm.at[:, pl.ds(pl.multiple_of(me * cb, LANES), cb)], w_own, ld_sem.at[3]),
        pltpu.make_async_copy(temp_hbm, temp_ref, ld_sem.at[4]),
        pltpu.make_async_copy(tgt_hbm, tgt_ref, ld_sem.at[5]),
    ]
    for c in loads:
        c.start()

    barrier = pltpu.get_barrier_semaphore()
    for j in range(1, nh):
        pl.semaphore_signal(barrier, inc=1, device_id={"hid": lax.rem(me + j, nh)},
                            device_id_type=MESH)
    for j in range(1, nv):
        pl.semaphore_signal(barrier, inc=1, device_id={"vocab": lax.rem(vi + j, nv)},
                            device_id_type=MESH)
    pl.semaphore_wait(barrier, nh - 1 + nv - 1)

    to_dn, to_up = {"hid": dn}, {"hid": up}
    mine = rws(vi * piece, piece)
    hy = [rdma(h_hbm.at[mine], h_nb.at[0, mine], hy_ss.at[0], hy_rs.at[0], to_dn),
          rdma(h_hbm.at[mine], h_nb.at[1, mine], hy_ss.at[1], hy_rs.at[1], to_up)]
    leaf = [rdma(w_hbm.at[:, tok(far, 0)], w_leaf.at[0], leaf_ss.at[0], leaf_rs.at[0], to_dn),
            rdma(w_hbm.at[:, tok(far, 1)], w_leaf.at[1], leaf_ss.at[1], leaf_rs.at[1], to_up)]
    direct = [rdma(w_hbm.at[:, tok(up, 0)], w_dir.at[0], dir_ss.at[0], dir_rs.at[0], to_up),
              rdma(w_hbm.at[:, tok(dn, 1)], w_dir.at[1], dir_ss.at[1], dir_rs.at[1], to_dn)]
    for c in hy + leaf:
        c.start()

    to_nxt, to_prv, to_mate = {"vocab": nxt}, {"vocab": prv}, {"vocab": mate}

    def hx(a, k, at, dev):
        return rdma(h_nb.at[a, at], h_nb.at[a, at], hx_ss.at[a, k], hx_rs.at[a, k], dev)

    from_prv = rws(prv * piece, piece)
    from_nxt = rws(nxt * piece, piece)
    opp_all = rws(opp * piece, piece)
    started = []

    def go(c):
        c.start()
        started.append(c)

    for a in range(2):
        hy[a].wait_recv()
        go(hx(a, 0, mine, to_nxt))
        go(hx(a, 1, mine, to_prv))
        go(hx(a, 4, mine, to_mate))
    for c in direct:
        c.start()

    for c in loads:
        c.wait()

    def own(i, _):
        at = rws(i * R, R)
        x = h_own[at]
        for p in range(2):
            s_send[p, at] = jnp.dot(x, w_sum[p], preferred_element_type=jnp.float32)
        for p in range(2):
            z_buf[at, p * hc:(p + 1) * hc] = jnp.dot(
                x, w_own[:, p * hc:(p + 1) * hc], preferred_element_type=jnp.float32)
        return 0

    lax.fori_loop(0, nr, own, 0)

    for a in range(2):
        hx(a, 0, from_prv, to_nxt).wait_recv()
        lo = rws(prv * piece, half)
        go(hx(a, 2, lo, to_nxt))
        go(hx(a, 5, from_prv, to_mate))
        hx(a, 1, from_nxt, to_prv).wait_recv()
        hi = rws(nxt * piece + half, half)
        go(hx(a, 3, hi, to_prv))
        go(hx(a, 6, from_nxt, to_mate))
    for a in range(2):
        hx(a, 2, rws(opp * piece, half), to_nxt).wait_recv()
        hx(a, 3, rws(opp * piece + half, half), to_prv).wait_recv()
        go(hx(a, 7, opp_all, to_mate))
    for a in range(2):
        for k in range(4, 8):
            hx(a, k, mine, to_mate).wait_recv()

    for c in leaf:
        c.wait_recv()

    def sum_copy(p, i):
        at = rws(i * R, R)
        return rdma(s_send.at[p, at], s_recv.at[p, at], sum_ss.at[p, i], sum_rs.at[p, i],
                    to_dn if p == 0 else to_up)

    def add_leaf(i, _):
        at = rws(i * R, R)
        for p in range(2):
            s_send[p, at] = s_send[p, at] + jnp.dot(
                h_nb[p, at], w_leaf[p], preferred_element_type=jnp.float32)
        for p in range(2):
            sum_copy(p, i).start()
        return 0

    lax.fori_loop(0, nr, add_leaf, 0)

    for c in direct:
        c.wait_recv()

    tri = (lax.broadcasted_iota(jnp.int32, (TRI, TRI), 0)
           <= lax.broadcasted_iota(jnp.int32, (TRI, TRI), 1)).astype(jnp.bfloat16)
    col = lax.broadcasted_iota(jnp.int32, (R, TRI), 1).astype(jnp.float32)
    lane = lax.broadcasted_iota(jnp.int32, (R, LANES), 1)
    first_tok = ((vi * nh + me) * cb).astype(jnp.float32)

    def by_row(v):
        return jnp.broadcast_to(v, (LANES, R)).T

    def finish(start, scale, off):
        a, b = by_row(scale), by_row(off)
        for j in range(cb // LANES):
            sl = slice(j * LANES, (j + 1) * LANES)
            z_buf[start:start + R, sl] = z_buf[start:start + R, sl] * a + b

    def softmax(i, sy, slot, k):
        at = rws(i * R, R)
        for p in range(2):
            sl = slice(p * hc, (p + 1) * hc)
            z_buf[at, sl] = z_buf[at, sl] + jnp.dot(
                h_nb[1 - p, at], w_dir[p], preferred_element_type=jnp.float32)
        temp = jnp.concatenate([by_row(temp_ref[pl.ds(i, 1)])] * (TRI // LANES), axis=1)
        tgt = jnp.concatenate(
            [by_row(tgt_ref[pl.ds(i, 1)].astype(jnp.float32) - first_tok)] * (TRI // LANES), axis=1)
        for p in range(2):
            sum_copy(p, i).wait_recv()
        m = None
        zs = []
        for b in range(cb // TRI):
            p, o = divmod(b * TRI, hc)
            z = (z_buf[at, b * TRI:(b + 1) * TRI] + s_recv[p, at, o:o + TRI]) * temp
            zs.append(z)
            m = z if m is None else jnp.maximum(m, z)
        m = jnp.max(m, axis=1, keepdims=True)
        total = jnp.zeros((R, TRI), jnp.float32)
        picked = jnp.zeros((R, TRI), jnp.float32)
        for b in range(cb // TRI):
            e = jnp.exp(zs[b] - m)
            z_buf[at, b * TRI:(b + 1) * TRI] = e
            total = total + e
            picked = picked + jnp.where(col + float(b * TRI) <= tgt, e, 0.0)
        s = jnp.sum(total, axis=1, keepdims=True)
        t = jnp.sum(picked, axis=1, keepdims=True)
        st = jnp.where(lane == 0, m, jnp.where(lane == 1, s, jnp.where(lane == 2, t, 0.0))).T
        for q in range(3):
            sy[slot, q, pl.ds(k, 1)] = st[q:q + 1]

    def running_sum(i):
        at = rws(i * R, R)
        carry = jnp.zeros((R, 1), jnp.float32)
        for b in range(cb // TRI):
            e = z_buf[at, b * TRI:(b + 1) * TRI]
            e1 = e.astype(jnp.bfloat16)
            r1 = e - e1.astype(jnp.float32)
            e2 = r1.astype(jnp.bfloat16)
            e3 = (r1 - e2.astype(jnp.float32)).astype(jnp.bfloat16)
            c = (jnp.dot(e3, tri, preferred_element_type=jnp.float32)
                 + jnp.dot(e2, tri, preferred_element_type=jnp.float32)
                 + jnp.dot(e1, tri, preferred_element_type=jnp.float32)) + carry
            z_buf[at, b * TRI:(b + 1) * TRI] = c
            carry = c[:, TRI - 1:TRI]

    na = nr - NB

    def stx(j):
        return rdma(sx_a.at[vi], sx_a.at[vi], stx_ss.at[j - 1], stx_rs.at[vi],
                    {"vocab": lax.rem(vi + j, nv)})

    def sty(j):
        return rdma(sy_out.at[j - 1], sy_a.at[me], sty_ss.at[j - 1], sty_rs.at[me],
                    {"hid": lax.rem(me + j, nh)})

    def merge_x():
        for j in range(1, nv):
            s = lax.rem(vi + j, nv)
            rdma(sx_a.at[s], sx_a.at[s], stx_ss.at[j - 1], stx_rs.at[s], to_nxt).wait_recv()
        big = sx_a[0, 0]
        for j in range(1, nv):
            big = jnp.maximum(big, sx_a[j, 0])
        zero = jnp.zeros_like(big)
        tot, low, hit, own_s = zero, zero, zero, zero
        for j in range(nv):
            f = jnp.exp(sx_a[j, 0] - big)
            s_j = sx_a[j, 1] * f
            low = low + jnp.where(j < vi, s_j, 0.0)
            own_s = own_s + jnp.where(j == vi, s_j, 0.0)
            tot = tot + s_j
            hit = hit + sx_a[j, 2] * f
        for q, v in enumerate((big, tot, hit, low)):
            sy_a[me, q] = v
        for j in range(1, nh):
            below = low + jnp.where(me < lax.rem(me + j, nh), own_s, 0.0)
            for q, v in enumerate((big, tot, hit, below)):
                sy_out[j - 1, q] = v
        for j in range(1, nh):
            sty(j).start()

    def merge_y():
        for j in range(1, nh):
            s = lax.rem(me + j, nh)
            rdma(sy_out.at[j - 1], sy_a.at[s], sty_ss.at[j - 1], sty_rs.at[s], to_up).wait_recv()
        big = sy_a[0, 0]
        for j in range(1, nh):
            big = jnp.maximum(big, sy_a[j, 0])
        zero = jnp.zeros_like(big)
        tot, low, hit = zero, zero, zero
        for j in range(nh):
            f = jnp.exp(sy_a[j, 0] - big)
            tot = tot + sy_a[j, 1] * f
            hit = hit + sy_a[j, 2] * f
            low = low + sy_a[j, 3] * f
        scale = jnp.exp(sx_a[vi, 0] - big) / tot
        off = low / tot
        hit_ref[0:na] = hit / tot
        for i in range(na):
            finish(i * R, scale[i:i + 1], off[i:i + 1])

    nd = nv * nh
    own_slot = vi * nh + me

    def peer(k):
        return lax.rem(vi + k // nh, nv), lax.rem(me + lax.rem(k, nh), nh)

    def sta(k):
        v, h = peer(k)
        return rdma(s_all.at[own_slot], s_all.at[own_slot], all_ss.at[k], all_rs.at[own_slot],
                    {"hid": h, "vocab": v})

    def send_all(k, _):
        sta(k).start()
        return 0

    def hear_all(k, _):
        v, h = peer(k)
        s = v * nh + h
        rdma(s_all.at[s], s_all.at[s], all_ss.at[k], all_rs.at[s], to_up).wait_recv()
        return 0

    def sent_all(k, _):
        sta(k).wait_send()
        return 0

    def merge_all():
        big = s_all[0, 0]
        for j in range(1, nd):
            big = jnp.maximum(big, s_all[j, 0])
        zero = jnp.zeros_like(big)
        tot, low, hit = zero, zero, zero
        for j in range(nd):
            f = jnp.exp(s_all[j, 0] - big)
            s_j = s_all[j, 1] * f
            low = low + jnp.where(j < own_slot, s_j, 0.0)
            tot = tot + s_j
            hit = hit + s_all[j, 2] * f
        hit_ref[na:nr] = hit / tot
        scale = jnp.exp(s_all[own_slot, 0] - big) / tot
        off = low / tot
        for i in range(NB):
            finish((na + i) * R, scale[i:i + 1], off[i:i + 1])

    def block(i, _):
        softmax(i, sx_a, vi, i)
        running_sum(i)
        return 0

    lax.fori_loop(0, na, block, 0)
    for j in range(1, nv):
        stx(j).start()

    def late_block(i, _):
        softmax(na + i, s_all, own_slot, i)
        running_sum(na + i)
        return 0

    lax.fori_loop(0, NB - 1, late_block, 0)
    merge_x()
    softmax(nr - 1, s_all, own_slot, NB - 1)
    for k in range(1, nd):
        send_all(k, 0)
    running_sum(nr - 1)

    for c in hy + leaf + direct + started:
        c.wait_send()

    def drain(i, _):
        for p in range(2):
            sum_copy(p, i).wait_send()
        return 0

    lax.fori_loop(0, nr, drain, 0)
    merge_y()
    lax.fori_loop(1, nd, hear_all, 0)
    merge_all()
    for j in range(1, nh):
        sty(j).wait_send()
    for j in range(1, nv):
        stx(j).wait_send()
    lax.fori_loop(1, nd, sent_all, 0)


def store_kernel(nc, c_ref, hit_ref, out_hbm, hit_hbm, sem):
    rows = c_ref.shape[0] // nc
    copies = [pltpu.make_async_copy(c_ref.at[i * rows:(i + 1) * rows],
                                    out_hbm.at[i * rows:(i + 1) * rows], sem.at[i])
              for i in range(nc)]
    copies.append(pltpu.make_async_copy(hit_ref, hit_hbm, sem.at[nc]))
    for c in copies:
        c.start()
    for c in copies:
        c.wait()


def solution(mesh):
    nh = mesh.shape["hid"]
    nv = mesh.shape["vocab"]

    def local_step(h, w, temp, tgt):
        rows, depth = h.shape
        cols = w.shape[1]
        cb = cols // nh
        hc = cb // 2
        nr = rows // R
        f32, bf16 = jnp.float32, jnp.bfloat16
        dma = pltpu.SemaphoreType.DMA
        vm = pl.BlockSpec(memory_space=pltpu.VMEM)
        hbm = pl.BlockSpec(memory_space=pltpu.HBM)
        row_stat = jax.ShapeDtypeStruct((nr, R), f32)
        cdf_out = jax.ShapeDtypeStruct((rows, cb), f32)
        table, hit = pl.pallas_call(
            functools.partial(head_kernel, nh, nv),
            name="head",
            out_shape=(cdf_out, row_stat),
            in_specs=[hbm, hbm, hbm, hbm],
            out_specs=(vm, vm),
            scratch_shapes=[
                pltpu.VMEM((rows, depth), bf16),
                pltpu.VMEM((2, rows, depth), bf16),
                pltpu.VMEM((2, depth, hc), bf16),
                pltpu.VMEM((depth, cb), bf16),
                pltpu.VMEM((2, depth, hc), bf16),
                pltpu.VMEM((2, depth, hc), bf16),
                pltpu.VMEM((2, rows, hc), f32),
                pltpu.VMEM((2, rows, hc), f32),
                pltpu.VMEM((nr, R), f32),
                pltpu.VMEM((nr, R), jnp.int32),
                pltpu.VMEM((nv, 3, nr - NB, R), f32),
                pltpu.VMEM((nh - 1, 4, nr - NB, R), f32),
                pltpu.VMEM((nh, 4, nr - NB, R), f32),
                pltpu.VMEM((nh * nv, 3, NB, R), f32),
                dma((6,)), dma((2,)), dma((2,)), dma((2, 8)), dma((2, 8)),
                dma((2,)), dma((2,)), dma((2,)), dma((2,)),
                dma((2, nr)), dma((2, nr)),
                dma((nh - 1,)), dma((nh,)), dma((nv - 1,)), dma((nv,)), dma((nh * nv,)), dma((nh * nv,)),
            ],
            cost_estimate=pl.CostEstimate(
                flops=2 * rows * depth * cols, bytes_accessed=2 * depth * (rows + cols) + 4 * rows * cb,
                transcendentals=rows * cb),
            compiler_params=pltpu.CompilerParams(
                collective_id=0, has_side_effects=True, vmem_limit_bytes=44 * 1024 * 1024),
        )(*[pltpu.with_memory_space_constraint(x, pltpu.HBM)
            for x in (h, w, temp.reshape(nr, R), tgt.reshape(nr, R))])
        cdf, ctgt = pl.pallas_call(
            functools.partial(store_kernel, NC),
            name="store",
            out_shape=(cdf_out, row_stat),
            in_specs=[vm, vm],
            out_specs=(hbm, hbm),
            scratch_shapes=[dma((NC + 1,))],
            compiler_params=pltpu.CompilerParams(vmem_limit_bytes=4 * 1024 * 1024),
        )(table, hit)
        return cdf, ctgt.reshape(rows)

    return jax.shard_map(
        local_step, mesh=mesh,
        in_specs=(P("data", "hid"), P("hid", "vocab"), P("data"), P("data")),
        out_specs=(P("data", ("vocab", "hid")), P("data")), check_vma=False)
```

```python
import functools

import jax
import jax.numpy as jnp
from jax import lax
from jax.experimental import pallas as pl
from jax.experimental.pallas import tpu as pltpu
from jax.sharding import PartitionSpec as P

MESH = pl.DeviceIdType.MESH
R = 128
LANES = 128
NC = 1
NB = 2
PARTS = ((0, 64), (64, 32), (96, 32))
TRI = 256


def head_kernel(nh, nv, h_hbm, w_hbm, temp_hbm, tgt_hbm,
                z_buf, hit_ref,
                h_own, h_nb, w_sum, w_own, w_leaf, w_dir, s_send, s_recv, temp_ref, tgt_ref,
                sx_a, sy_out, sy_a, s_all, st_buf,
                ld_sem, hy_ss, hy_rs, hx_ss, hx_rs, leaf_ss, leaf_rs, dir_ss, dir_rs,
                sum_ss, sum_rs, sty_ss, sty_rs, stx_ss, stx_rs, all_ss, all_rs):
    rows, depth = h_hbm.shape
    cb = w_hbm.shape[1] // nh
    hc = cb // 2
    nr = rows // R
    piece = rows // nv
    half = piece // 2

    me = lax.axis_index("hid")
    vi = lax.axis_index("vocab")
    up = lax.rem(me + 1, nh)
    dn = lax.rem(me + nh - 1, nh)
    far = lax.rem(me + 2, nh)
    nxt = lax.rem(vi + 2, nv)
    prv = lax.rem(vi + nv - 2, nv)
    opp = lax.rem(vi + 4, nv)
    mate = vi + 1 - 2 * lax.rem(vi, 2)

    def tok(d, part):
        return pl.ds(pl.multiple_of(d * cb + part * hc, LANES), hc)

    def rws(start, n):
        return pl.ds(pl.multiple_of(start, n), n)

    def rdma(src, dst, ss, rs, dev):
        return pltpu.make_async_remote_copy(
            src_ref=src, dst_ref=dst, send_sem=ss, recv_sem=rs,
            device_id=dev, device_id_type=MESH)

    loads = [
        pltpu.make_async_copy(h_hbm, h_own, ld_sem.at[0]),
        pltpu.make_async_copy(w_hbm.at[:, tok(dn, 0)], w_sum.at[0], ld_sem.at[1]),
        pltpu.make_async_copy(w_hbm.at[:, tok(up, 1)], w_sum.at[1], ld_sem.at[2]),
        pltpu.make_async_copy(
            w_hbm.at[:, pl.ds(pl.multiple_of(me * cb, LANES), cb)], w_own, ld_sem.at[3]),
        pltpu.make_async_copy(temp_hbm, temp_ref, ld_sem.at[4]),
        pltpu.make_async_copy(tgt_hbm, tgt_ref, ld_sem.at[5]),
    ]
    for c in loads:
        c.start()

    barrier = pltpu.get_barrier_semaphore()
    for j in range(1, nh):
        pl.semaphore_signal(barrier, inc=1, device_id={"hid": lax.rem(me + j, nh)},
                            device_id_type=MESH)
    for j in range(1, nv):
        pl.semaphore_signal(barrier, inc=1, device_id={"vocab": lax.rem(vi + j, nv)},
                            device_id_type=MESH)
    pl.semaphore_wait(barrier, nh - 1 + nv - 1)

    to_dn, to_up = {"hid": dn}, {"hid": up}
    mine = rws(vi * piece, piece)
    hy = [rdma(h_hbm.at[mine], h_nb.at[0, mine], hy_ss.at[0], hy_rs.at[0], to_dn),
          rdma(h_hbm.at[mine], h_nb.at[1, mine], hy_ss.at[1], hy_rs.at[1], to_up)]
    leaf = [rdma(w_hbm.at[:, tok(far, 0)], w_leaf.at[0], leaf_ss.at[0], leaf_rs.at[0], to_dn),
            rdma(w_hbm.at[:, tok(far, 1)], w_leaf.at[1], leaf_ss.at[1], leaf_rs.at[1], to_up)]
    direct = [rdma(w_hbm.at[:, tok(up, 0)], w_dir.at[0], dir_ss.at[0], dir_rs.at[0], to_up),
              rdma(w_hbm.at[:, tok(dn, 1)], w_dir.at[1], dir_ss.at[1], dir_rs.at[1], to_dn)]
    for c in hy + leaf:
        c.start()

    to_nxt, to_prv, to_mate = {"vocab": nxt}, {"vocab": prv}, {"vocab": mate}

    def hx(a, k, at, dev):
        return rdma(h_nb.at[a, at], h_nb.at[a, at], hx_ss.at[a, k], hx_rs.at[a, k], dev)

    from_prv = rws(prv * piece, piece)
    from_nxt = rws(nxt * piece, piece)
    opp_all = rws(opp * piece, piece)
    started = []

    def go(c):
        c.start()
        started.append(c)

    for a in range(2):
        hy[a].wait_recv()
        go(hx(a, 0, mine, to_nxt))
        go(hx(a, 1, mine, to_prv))
        go(hx(a, 4, mine, to_mate))
    for c in direct:
        c.start()

    for c in loads:
        c.wait()

    def own(i, _):
        at = rws(i * R, R)
        x = h_own[at]
        for p in range(2):
            s_send[p, at] = jnp.dot(x, w_sum[p], preferred_element_type=jnp.float32)
        for p in range(2):
            z_buf[at, p * hc:(p + 1) * hc] = jnp.dot(
                x, w_own[:, p * hc:(p + 1) * hc], preferred_element_type=jnp.float32)
        return 0

    lax.fori_loop(0, nr, own, 0)

    for a in range(2):
        hx(a, 0, from_prv, to_nxt).wait_recv()
        lo = rws(prv * piece, half)
        go(hx(a, 2, lo, to_nxt))
        go(hx(a, 5, from_prv, to_mate))
        hx(a, 1, from_nxt, to_prv).wait_recv()
        hi = rws(nxt * piece + half, half)
        go(hx(a, 3, hi, to_prv))
        go(hx(a, 6, from_nxt, to_mate))
    for a in range(2):
        hx(a, 2, rws(opp * piece, half), to_nxt).wait_recv()
        hx(a, 3, rws(opp * piece + half, half), to_prv).wait_recv()
        go(hx(a, 7, opp_all, to_mate))
    for a in range(2):
        for k in range(4, 8):
            hx(a, k, mine, to_mate).wait_recv()

    for c in leaf:
        c.wait_recv()

    last = nr - 1

    def sum_part(p, start, n, k):
        at = rws(start, n)
        return rdma(s_send.at[p, at], s_recv.at[p, at], sum_ss.at[p, k], sum_rs.at[p, k],
                    to_dn if p == 0 else to_up)

    def sum_copy(p, i):
        return sum_part(p, i * R, R, i)

    last_sums = [[sum_part(p, last * R + lo, n, last + k) for p in range(2)]
                 for k, (lo, n) in enumerate(PARTS)]

    def add_leaf(i):
        at = rws(i * R, R)
        for p in range(2):
            s_send[p, at] = s_send[p, at] + jnp.dot(
                h_nb[p, at], w_leaf[p], preferred_element_type=jnp.float32)

    def sums(i, _):
        add_leaf(i)
        for p in range(2):
            sum_copy(p, i).start()
        return 0

    lax.fori_loop(0, last, sums, 0)
    add_leaf(last)
    for pair in last_sums:
        for c in pair:
            c.start()

    for c in direct:
        c.wait_recv()

    tri = (lax.broadcasted_iota(jnp.int32, (TRI, TRI), 0)
           <= lax.broadcasted_iota(jnp.int32, (TRI, TRI), 1)).astype(jnp.bfloat16)
    col = lax.broadcasted_iota(jnp.int32, (R, TRI), 1).astype(jnp.float32)
    lane = lax.broadcasted_iota(jnp.int32, (R, LANES), 1)
    first_tok = ((vi * nh + me) * cb).astype(jnp.float32)

    def by_row(v):
        return jnp.broadcast_to(v, (LANES, R)).T

    def finish(start, scale, off):
        a, b = by_row(scale), by_row(off)
        for j in range(cb // LANES):
            sl = slice(j * LANES, (j + 1) * LANES)
            z_buf[start:start + R, sl] = z_buf[start:start + R, sl] * a + b

    def row_values(i):
        temp = jnp.concatenate([by_row(temp_ref[pl.ds(i, 1)])] * (TRI // LANES), axis=1)
        tgt = jnp.concatenate(
            [by_row(tgt_ref[pl.ds(i, 1)].astype(jnp.float32) - first_tok)] * (TRI // LANES), axis=1)
        return temp, tgt

    def add_direct(i):
        at = rws(i * R, R)
        for p in range(2):
            sl = slice(p * hc, (p + 1) * hc)
            z_buf[at, sl] = z_buf[at, sl] + jnp.dot(
                h_nb[1 - p, at], w_dir[p], preferred_element_type=jnp.float32)

    def exps(start, lo, n, temp, tgt):
        at = rws(start, n)
        temp, tgt = temp[lo:lo + n], tgt[lo:lo + n]
        m = None
        zs = []
        for b in range(cb // TRI):
            p, o = divmod(b * TRI, hc)
            z = (z_buf[at, b * TRI:(b + 1) * TRI] + s_recv[p, at, o:o + TRI]) * temp
            zs.append(z)
            m = z if m is None else jnp.maximum(m, z)
        m = jnp.max(m, axis=1, keepdims=True)
        total = jnp.zeros((n, TRI), jnp.float32)
        picked = jnp.zeros((n, TRI), jnp.float32)
        for b in range(cb // TRI):
            e = jnp.exp(zs[b] - m)
            z_buf[at, b * TRI:(b + 1) * TRI] = e
            total = total + e
            picked = picked + jnp.where(col[:n] + float(b * TRI) <= tgt, e, 0.0)
        s = jnp.sum(total, axis=1, keepdims=True)
        t = jnp.sum(picked, axis=1, keepdims=True)
        ln = lane[:n]
        st_buf[lo:lo + n] = jnp.where(ln == 0, m, jnp.where(ln == 1, s, jnp.where(ln == 2, t, 0.0)))

    def publish(sy, slot, k):
        st = st_buf[...].T
        for q in range(3):
            sy[slot, q, pl.ds(k, 1)] = st[q:q + 1]

    def softmax(i, sy, slot, k):
        add_direct(i)
        temp, tgt = row_values(i)
        for p in range(2):
            sum_copy(p, i).wait_recv()
        exps(i * R, 0, R, temp, tgt)
        publish(sy, slot, k)

    def softmax_last(sy, slot, k):
        add_direct(last)
        temp, tgt = row_values(last)
        for (lo, n), pair in zip(PARTS, last_sums):
            for c in pair:
                c.wait_recv()
            exps(last * R + lo, lo, n, temp, tgt)
        publish(sy, slot, k)

    def running_sum(i):
        at = rws(i * R, R)
        carry = jnp.zeros((R, 1), jnp.float32)
        for b in range(cb // TRI):
            e = z_buf[at, b * TRI:(b + 1) * TRI]
            e1 = e.astype(jnp.bfloat16)
            r1 = e - e1.astype(jnp.float32)
            e2 = r1.astype(jnp.bfloat16)
            e3 = (r1 - e2.astype(jnp.float32)).astype(jnp.bfloat16)
            c = (jnp.dot(e3, tri, preferred_element_type=jnp.float32)
                 + jnp.dot(e2, tri, preferred_element_type=jnp.float32)
                 + jnp.dot(e1, tri, preferred_element_type=jnp.float32)) + carry
            z_buf[at, b * TRI:(b + 1) * TRI] = c
            carry = c[:, TRI - 1:TRI]

    na = nr - NB

    def stx(j):
        return rdma(sx_a.at[vi], sx_a.at[vi], stx_ss.at[j - 1], stx_rs.at[vi],
                    {"vocab": lax.rem(vi + j, nv)})

    def sty(j):
        return rdma(sy_out.at[j - 1], sy_a.at[me], sty_ss.at[j - 1], sty_rs.at[me],
                    {"hid": lax.rem(me + j, nh)})

    def merge_x():
        for j in range(1, nv):
            s = lax.rem(vi + j, nv)
            rdma(sx_a.at[s], sx_a.at[s], stx_ss.at[j - 1], stx_rs.at[s], to_nxt).wait_recv()
        big = sx_a[0, 0]
        for j in range(1, nv):
            big = jnp.maximum(big, sx_a[j, 0])
        zero = jnp.zeros_like(big)
        tot, low, hit, own_s = zero, zero, zero, zero
        for j in range(nv):
            f = jnp.exp(sx_a[j, 0] - big)
            s_j = sx_a[j, 1] * f
            low = low + jnp.where(j < vi, s_j, 0.0)
            own_s = own_s + jnp.where(j == vi, s_j, 0.0)
            tot = tot + s_j
            hit = hit + sx_a[j, 2] * f
        for q, v in enumerate((big, tot, hit, low)):
            sy_a[me, q] = v
        for j in range(1, nh):
            below = low + jnp.where(me < lax.rem(me + j, nh), own_s, 0.0)
            for q, v in enumerate((big, tot, hit, below)):
                sy_out[j - 1, q] = v
        for j in range(1, nh):
            sty(j).start()

    def merge_y():
        for j in range(1, nh):
            s = lax.rem(me + j, nh)
            rdma(sy_out.at[j - 1], sy_a.at[s], sty_ss.at[j - 1], sty_rs.at[s], to_up).wait_recv()
        big = sy_a[0, 0]
        for j in range(1, nh):
            big = jnp.maximum(big, sy_a[j, 0])
        zero = jnp.zeros_like(big)
        tot, low, hit = zero, zero, zero
        for j in range(nh):
            f = jnp.exp(sy_a[j, 0] - big)
            tot = tot + sy_a[j, 1] * f
            hit = hit + sy_a[j, 2] * f
            low = low + sy_a[j, 3] * f
        scale = jnp.exp(sx_a[vi, 0] - big) / tot
        off = low / tot
        hit_ref[0:na] = hit / tot
        for i in range(na):
            finish(i * R, scale[i:i + 1], off[i:i + 1])

    nd = nv * nh
    own_slot = vi * nh + me

    def hops(k):
        v, h = k // nh, k % nh
        return min((v + 1) // 2, (nv - v + 1) // 2) + min(h, nh - h)

    near_first = sorted(range(1, nd), key=hops)

    def peer(k):
        return lax.rem(vi + k // nh, nv), lax.rem(me + k % nh, nh)

    def sta(k):
        v, h = peer(k)
        return rdma(s_all.at[own_slot], s_all.at[own_slot], all_ss.at[k], all_rs.at[own_slot],
                    {"hid": h, "vocab": v})

    def hear(k):
        v, h = peer(k)
        s = v * nh + h
        rdma(s_all.at[s], s_all.at[s], all_ss.at[k], all_rs.at[s], to_up).wait_recv()

    def merge_all():
        big = s_all[0, 0]
        for j in range(1, nd):
            big = jnp.maximum(big, s_all[j, 0])
        zero = jnp.zeros_like(big)
        tot, low, hit = zero, zero, zero
        for j in range(nd):
            f = jnp.exp(s_all[j, 0] - big)
            s_j = s_all[j, 1] * f
            low = low + jnp.where(j < own_slot, s_j, 0.0)
            tot = tot + s_j
            hit = hit + s_all[j, 2] * f
        hit_ref[na:nr] = hit / tot
        scale = jnp.exp(s_all[own_slot, 0] - big) / tot
        off = low / tot
        for i in range(NB):
            finish((na + i) * R, scale[i:i + 1], off[i:i + 1])

    def block(i, _):
        softmax(i, sx_a, vi, i)
        running_sum(i)
        return 0

    lax.fori_loop(0, na, block, 0)
    for j in range(1, nv):
        stx(j).start()

    def late_block(i, _):
        softmax(na + i, s_all, own_slot, i)
        running_sum(na + i)
        return 0

    lax.fori_loop(0, NB - 1, late_block, 0)
    merge_x()
    softmax_last(s_all, own_slot, NB - 1)
    for k in reversed(near_first):
        sta(k).start()
    running_sum(last)

    for c in hy + leaf + direct + started:
        c.wait_send()

    def drain(i, _):
        for p in range(2):
            sum_copy(p, i).wait_send()
        return 0

    lax.fori_loop(0, last, drain, 0)
    for pair in last_sums:
        for c in pair:
            c.wait_send()
    for j in range(1, nv):
        stx(j).wait_send()
    merge_y()
    for j in range(1, nh):
        sty(j).wait_send()
    for k in near_first:
        sta(k).wait_send()
    for k in near_first:
        hear(k)
    merge_all()


def store_kernel(nc, c_ref, hit_ref, out_hbm, hit_hbm, sem):
    rows = c_ref.shape[0] // nc
    copies = [pltpu.make_async_copy(c_ref.at[i * rows:(i + 1) * rows],
                                    out_hbm.at[i * rows:(i + 1) * rows], sem.at[i])
              for i in range(nc)]
    copies.append(pltpu.make_async_copy(hit_ref, hit_hbm, sem.at[nc]))
    for c in copies:
        c.start()
    for c in copies:
        c.wait()


def solution(mesh):
    nh = mesh.shape["hid"]
    nv = mesh.shape["vocab"]

    def local_step(h, w, temp, tgt):
        rows, depth = h.shape
        cols = w.shape[1]
        cb = cols // nh
        hc = cb // 2
        nr = rows // R
        f32, bf16 = jnp.float32, jnp.bfloat16
        dma = pltpu.SemaphoreType.DMA
        vm = pl.BlockSpec(memory_space=pltpu.VMEM)
        hbm = pl.BlockSpec(memory_space=pltpu.HBM)
        row_stat = jax.ShapeDtypeStruct((nr, R), f32)
        cdf_out = jax.ShapeDtypeStruct((rows, cb), f32)
        table, hit = pl.pallas_call(
            functools.partial(head_kernel, nh, nv),
            name="head",
            out_shape=(cdf_out, row_stat),
            in_specs=[hbm, hbm, hbm, hbm],
            out_specs=(vm, vm),
            scratch_shapes=[
                pltpu.VMEM((rows, depth), bf16),
                pltpu.VMEM((2, rows, depth), bf16),
                pltpu.VMEM((2, depth, hc), bf16),
                pltpu.VMEM((depth, cb), bf16),
                pltpu.VMEM((2, depth, hc), bf16),
                pltpu.VMEM((2, depth, hc), bf16),
                pltpu.VMEM((2, rows, hc), f32),
                pltpu.VMEM((2, rows, hc), f32),
                pltpu.VMEM((nr, R), f32),
                pltpu.VMEM((nr, R), jnp.int32),
                pltpu.VMEM((nv, 3, nr - NB, R), f32),
                pltpu.VMEM((nh - 1, 4, nr - NB, R), f32),
                pltpu.VMEM((nh, 4, nr - NB, R), f32),
                pltpu.VMEM((nh * nv, 3, NB, R), f32),
                pltpu.VMEM((R, LANES), f32),
                dma((6,)), dma((2,)), dma((2,)), dma((2, 8)), dma((2, 8)),
                dma((2,)), dma((2,)), dma((2,)), dma((2,)),
                dma((2, nr - 1 + len(PARTS))), dma((2, nr - 1 + len(PARTS))),
                dma((nh - 1,)), dma((nh,)), dma((nv - 1,)), dma((nv,)), dma((nh * nv,)), dma((nh * nv,)),
            ],
            cost_estimate=pl.CostEstimate(
                flops=2 * rows * depth * cols, bytes_accessed=2 * depth * (rows + cols) + 4 * rows * cb,
                transcendentals=rows * cb),
            compiler_params=pltpu.CompilerParams(
                collective_id=0, has_side_effects=True, vmem_limit_bytes=44 * 1024 * 1024),
        )(*[pltpu.with_memory_space_constraint(x, pltpu.HBM)
            for x in (h, w, temp.reshape(nr, R), tgt.reshape(nr, R))])
        cdf, ctgt = pl.pallas_call(
            functools.partial(store_kernel, NC),
            name="store",
            out_shape=(cdf_out, row_stat),
            in_specs=[vm, vm],
            out_specs=(hbm, hbm),
            scratch_shapes=[dma((NC + 1,))],
            compiler_params=pltpu.CompilerParams(vmem_limit_bytes=4 * 1024 * 1024),
        )(table, hit)
        return cdf, ctgt.reshape(rows)

    return jax.shard_map(
        local_step, mesh=mesh,
        in_specs=(P("data", "hid"), P("hid", "vocab"), P("data"), P("data")),
        out_specs=(P("data", ("vocab", "hid")), P("data")), check_vma=False)
```
